8 devices in a mesh: dp: 1 (over z), tp: 2 (over y), sp: 4 (over x, core).
Axes of the slice: x: 2, y: 2, z: 1, core: 2. Of those that a mesh axis runs over, the one named last changes fastest.
Arguments:
- x: bfloat16 [4096, 3584], P(('dp', 'sp'))
- pos: int32 [4096], P(('dp', 'sp'))
- k_hist: bfloat16 [3, 8192, 4, 128], P(None, ('dp', 'sp'), 'tp')
- v_hist: bfloat16 [3, 8192, 4, 128], P(None, ('dp', 'sp'), 'tp')
- wq: bfloat16 [3, 3584, 3584], P(None, None, 'tp')
- wk: bfloat16 [3, 3584, 512], P(None, None, 'tp')
- wv: bfloat16 [3, 3584, 512], P(None, None, 'tp')
- wo: bfloat16 [3, 3584, 3584], P(None, 'tp')
- wg: bfloat16 [3, 3584, 18944], P(None, None, 'tp')
- wu: bfloat16 [3, 3584, 18944], P(None, None, 'tp')
- wd: bfloat16 [3, 18944, 3584], P(None, 'tp')
- g1: bfloat16 [3, 3584], replicated
- g2: bfloat16 [3, 3584], replicated
Outputs:
- output 1: bfloat16 [4096, 3584], P(('dp', 'sp'))
- output 2: bfloat16 [3, 4096, 4, 128], P(None, ('dp', 'sp'), 'tp')
- output 3: bfloat16 [3, 4096, 4, 128], P(None, ('dp', 'sp'), 'tp')
All inputs are finite; a program needn't handle non-finite values.
Results may differ from the reference program's by a relative error of at most 0.02.
Values are sent between devices in bfloat16 or wider.
A program may use at most 2.75 GiB of HBM per device.

```python
import jax
import jax.numpy as jnp
from jax import lax

D = 3584
HEADS = 28
KV_HEADS = 4
HEAD = 128
FF = 18944
S = 4096
HIST = 8192
LAYERS = 3
QBLK = 32
EPS = 1e-5
ROPE_THETA = 500000.0


def setup_inputs(seed: int = 0, part: int = 0) -> dict:
    key = jax.random.PRNGKey(seed)
    ks = jax.random.split(key, 9)
    kp = jax.random.split(jax.random.fold_in(key, part), 4)
    f32 = jnp.float32

    def w(k, shape, fan_in, gain=1.0):
        return (jax.random.normal(k, shape, f32) * (gain * fan_in ** -0.5)).astype(jnp.bfloat16)

    off = jax.random.randint(kp[1], (), 0, 1024)
    kvshape = (LAYERS, HIST, KV_HEADS, HEAD)
    return {
        'x': jax.random.normal(kp[0], (S, D), f32).astype(jnp.bfloat16),
        'pos': (HIST + off + jnp.arange(S)).astype(jnp.int32),
        'k_hist': jax.random.normal(kp[2], kvshape, f32).astype(jnp.bfloat16),
        'v_hist': jax.random.normal(kp[3], kvshape, f32).astype(jnp.bfloat16),
        'wq': w(ks[0], (LAYERS, D, HEADS * HEAD), D, 3.0),
        'wk': w(ks[1], (LAYERS, D, KV_HEADS * HEAD), D),
        'wv': w(ks[2], (LAYERS, D, KV_HEADS * HEAD), D),
        'wo': w(ks[3], (LAYERS, HEADS * HEAD, D), HEADS * HEAD),
        'wg': w(ks[4], (LAYERS, D, FF), D),
        'wu': w(ks[5], (LAYERS, D, FF), D),
        'wd': w(ks[6], (LAYERS, FF, D), FF),
        'g1': (1.0 + 0.2 * jax.random.normal(ks[7], (LAYERS, D), f32)).astype(jnp.bfloat16),
        'g2': (1.0 + 0.2 * jax.random.normal(ks[8], (LAYERS, D), f32)).astype(jnp.bfloat16),
    }


def rmsnorm(x, g):
    xf = x.astype(jnp.float32)
    r = lax.rsqrt(jnp.mean(xf * xf, axis=-1, keepdims=True) + EPS)
    return (xf * r * g.astype(jnp.float32)).astype(jnp.bfloat16)


def rope(t, pos):
    half = t.shape[-1] // 2
    inv = ROPE_THETA ** (-(jnp.arange(half, dtype=jnp.float32) * (2.0 / t.shape[-1])))
    ang = pos.astype(jnp.float32)[..., None] * inv
    c = jnp.cos(ang)[..., None, :]
    s = jnp.sin(ang)[..., None, :]
    tf = t.astype(jnp.float32)
    t1 = tf[..., :half]
    t2 = tf[..., half:]
    return jnp.concatenate([t1 * c - t2 * s, t2 * c + t1 * s], axis=-1).astype(jnp.bfloat16)


def attention(q, k, v):
    g = HEADS // KV_HEADS
    kf = k.astype(jnp.float32)
    vf = v.astype(jnp.float32)
    qb = q.reshape(S // QBLK, QBLK, KV_HEADS, g, HEAD)
    kidx = jnp.arange(HIST + S)

    def blk(args):
        i, qq = args
        s = jnp.einsum('qkgd,tkd->qkgt', qq.astype(jnp.float32), kf) * HEAD ** -0.5
        qidx = HIST + i * QBLK + jnp.arange(QBLK)
        mask = (kidx[None, :] <= qidx[:, None])[:, None, None, :]
        s = jnp.where(mask, s, -jnp.inf)
        p = jax.nn.softmax(s, axis=-1).astype(jnp.bfloat16)
        o = jnp.einsum('qkgt,tkd->qkgd', p.astype(jnp.float32), vf)
        return o.astype(jnp.bfloat16)

    o = lax.map(blk, (jnp.arange(S // QBLK), qb))
    return o.reshape(S, HEADS * HEAD)


def reference(x, pos, k_hist, v_hist, wq, wk, wv, wo, wg, wu, wd, g1, g2):
    def layer(x, w):
        kh, vh, wq_, wk_, wv_, wo_, wg_, wu_, wd_, g1_, g2_ = w
        h = rmsnorm(x, g1_)
        q = jnp.dot(h, wq_, preferred_element_type=jnp.float32).astype(jnp.bfloat16).reshape(S, HEADS, HEAD)
        k = jnp.dot(h, wk_, preferred_element_type=jnp.float32).astype(jnp.bfloat16).reshape(S, KV_HEADS, HEAD)
        v = jnp.dot(h, wv_, preferred_element_type=jnp.float32).astype(jnp.bfloat16).reshape(S, KV_HEADS, HEAD)
        q = rope(q, pos)
        k = rope(k, pos)
        a = attention(q, jnp.concatenate([kh, k], axis=0), jnp.concatenate([vh, v], axis=0))
        x = x + jnp.dot(a, wo_, preferred_element_type=jnp.float32).astype(jnp.bfloat16)
        h2 = rmsnorm(x, g2_)
        ga = jnp.dot(h2, wg_, preferred_element_type=jnp.float32).astype(jnp.bfloat16)
        up = jnp.dot(h2, wu_, preferred_element_type=jnp.float32).astype(jnp.bfloat16)
        u = (jax.nn.silu(ga.astype(jnp.float32)) * up.astype(jnp.float32)).astype(jnp.bfloat16)
        x = x + jnp.dot(u, wd_, preferred_element_type=jnp.float32).astype(jnp.bfloat16)
        return x, (k, v)

    x, (kn, vn) = lax.scan(layer, x, (k_hist, v_hist, wq, wk, wv, wo, wg, wu, wd, g1, g2))
    return x, kn, vn
```

```python
import functools

import jax
import jax.numpy as jnp
from jax import lax
from jax.experimental import pallas as pl
from jax.experimental.pallas import tpu as pltpu
from jax.sharding import PartitionSpec as P

EPS = 1e-5
ROPE_THETA = 500000.0
LOG2E = 1.4426950408889634
NT = (((1,), (1,)), ((), ()))
F32 = jnp.float32
BF16 = jnp.bfloat16
VMEM_LIMIT = 60 * 2**20
TB = 256
CB = 256
OB = 512
DB = 512
HCHUNK = 2048
UNROLL = 3


def params(n=1):
    return pltpu.CompilerParams(vmem_limit_bytes=VMEM_LIMIT, dimension_semantics=("arbitrary",) * n)


def cost(flops, nbytes):
    return pl.CostEstimate(flops=int(flops), bytes_accessed=int(nbytes), transcendentals=0)


def norm_into(h_ref, x_ref, g_ref):
    xf = x_ref[...].astype(F32)
    r = lax.rsqrt(jnp.mean(xf * xf, axis=-1, keepdims=True) + EPS)
    h_ref[...] = (xf * r * g_ref[0].astype(F32)).astype(BF16)


def qkv_kernel(x_ref, g_ref, cos_ref, sin_ref, wq_ref, wk_ref, wv_ref, q_ref, kv_ref, h_ref, *, dh, nk):
    i = pl.program_id(0)

    def rope(t):
        t = t.astype(BF16).astype(F32)
        return (t * cos_ref[...] + pltpu.roll(t, dh // 2, 1) * sin_ref[...]).astype(BF16)

    @pl.when(i == 0)
    def _():
        norm_into(h_ref, x_ref, g_ref)
        y = jnp.dot(h_ref[...], wk_ref[0], preferred_element_type=F32)
        z = jnp.dot(h_ref[...], wv_ref[0], preferred_element_type=F32)
        for j in range(nk):
            kv_ref[0, j] = rope(y[:, j * dh:(j + 1) * dh])
            kv_ref[1, j] = z[:, j * dh:(j + 1) * dh].astype(BF16)

    @pl.when(i > 0)
    def _():
        y = jnp.dot(h_ref[...], wq_ref[0], preferred_element_type=F32)
        for j in range(CB // dh):
            q_ref[j] = rope(y[:, j * dh:(j + 1) * dh])


def qkv(l, x, g, cos, sin, wq, wk, wv, dh):
    n, d = x.shape
    cq, ck = wq.shape[-1], wk.shape[-1]
    nk = ck // dh
    nb = cq // CB
    qi = lambda i: jnp.maximum(i - 1, 0)
    return pl.pallas_call(
        functools.partial(qkv_kernel, dh=dh, nk=nk),
        grid=(nb + 1,),
        in_specs=[
            pl.BlockSpec((n, d), lambda i: (0, 0)),
            pl.BlockSpec((1, 1, d), lambda i: (l, 0, 0)),
            pl.BlockSpec((n, dh), lambda i: (0, 0)),
            pl.BlockSpec((n, dh), lambda i: (0, 0)),
            pl.BlockSpec((1, d, CB), lambda i: (l, 0, qi(i))),
            pl.BlockSpec((1, d, ck), lambda i: (l, 0, 0)),
            pl.BlockSpec((1, d, ck), lambda i: (l, 0, 0)),
        ],
        out_specs=[
            pl.BlockSpec((CB // dh, n, dh), lambda i: (qi(i), 0, 0)),
            pl.BlockSpec((2, nk, n, dh), lambda i: (0, 0, 0, 0)),
        ],
        out_shape=[
            jax.ShapeDtypeStruct((cq // dh, n, dh), BF16),
            jax.ShapeDtypeStruct((2, nk, n, dh), BF16),
        ],
        scratch_shapes=[pltpu.VMEM((n, d), BF16)],
        compiler_params=params(),
        cost_estimate=cost(2 * n * d * (cq + 2 * ck), 2 * d * (cq + 2 * ck)),
        name='qkv',
    )(x, g, cos, sin, wq, wk, wv)


def softmax_step(q, k, v, m_ref, l_ref, acc_ref, c, first=False, mask=None):
    s = lax.dot_general(q, k, NT, preferred_element_type=F32)
    if mask is not None:
        s = jnp.where(mask, s, -jnp.inf)
    dh = acc_ref.shape[-1]
    shape = acc_ref.shape
    rows = s.shape[0]
    mx = jnp.max(s, axis=1, keepdims=True)
    if first:
        mn = jnp.broadcast_to(mx, (rows, dh))
    else:
        mp = m_ref[...].reshape(rows, dh)
        mn = jnp.maximum(mp, mx)
        a = jnp.exp2((mp - mn) * c)
    m_ref[...] = mn.reshape(shape)
    nb = s.shape[1] // dh
    p = jnp.exp2((s - jnp.concatenate([mn] * nb, axis=1)) * c)
    ls = p[:, :dh]
    for b in range(1, nb):
        ls = ls + p[:, b * dh:(b + 1) * dh]
    o = jnp.dot(p.astype(BF16), v, preferred_element_type=F32)
    if not first:
        ls = l_ref[...].reshape(rows, dh) * a + ls
        o = acc_ref[...].reshape(rows, dh) * a + o
    l_ref[...] = ls.reshape(shape)
    acc_ref[...] = o.reshape(shape)


def hist_kernel(q_ref, k_ref, v_ref, m_ref, l_ref, acc_ref, *, c, chunk):
    g, tb, dh = q_ref.shape
    q = q_ref[...].reshape(g * tb, dh)
    for_sp, per = k_ref.shape[0], k_ref.shape[3] // chunk
    softmax_step(q, k_ref[0, 0, 0, :chunk], v_ref[0, 0, 0, :chunk], m_ref, l_ref, acc_ref, c, first=True)

    def body(j, _):
        a = j // per
        rows = pl.ds(pl.multiple_of((j - a * per) * chunk, chunk), chunk)
        softmax_step(q, k_ref[a, 0, 0, rows], v_ref[a, 0, 0, rows], m_ref, l_ref, acc_ref, c)
        return 0

    lax.fori_loop(1, for_sp * per, body, 0, unroll=UNROLL)


def hist_attn(q, kv, c):
    hq, n, dh = q.shape
    sp, _, nk, t, _ = kv.shape
    g = hq // nk
    st = pl.BlockSpec((g, TB, dh), lambda h, i: (h, i, 0))
    sd = jax.ShapeDtypeStruct((hq, n, dh), F32)
    return pl.pallas_call(
        functools.partial(hist_kernel, c=c, chunk=min(HCHUNK, t)),
        grid=(nk, n // TB),
        in_specs=[
            st,
            pl.BlockSpec((sp, 1, 1, t, dh), lambda h, i: (0, 0, h, 0, 0)),
            pl.BlockSpec((sp, 1, 1, t, dh), lambda h, i: (0, 1, h, 0, 0)),
        ],
        out_specs=[st, st, st],
        out_shape=[sd, sd, sd],
        compiler_params=params(2),
        cost_estimate=cost(8 * hq * n * sp * t * dh, 3 * hq * n * dh * 4),
        name='hist_attn',
    )(q, kv, kv)


def new_kernel(idx_ref, q_ref, k_ref, v_ref, m0_ref, l0_ref, acc0_ref, o_ref, m_ref, l_ref, acc_ref, *, c):
    g, tb, dh = q_ref.shape
    n = k_ref.shape[3]
    r = idx_ref[0]
    half = idx_ref[1]
    q = q_ref[...].reshape(g * tb, dh)
    m_ref[...] = m0_ref[...]
    l_ref[...] = l0_ref[...]
    acc_ref[...] = acc0_ref[...]

    def body(j, _):
        softmax_step(q, k_ref[j, 0, 0], v_ref[j, 0, 0], m_ref, l_ref, acc_ref, c)
        return 0

    lax.fori_loop(0, r, body, 0)
    row0 = half * (n // 2) + pl.program_id(1) * tb

    def diagonal(keys):
        shape = (g, tb, keys)
        ti = lax.broadcasted_iota(jnp.int32, shape, 1).reshape(g * tb, keys) + row0
        ki = lax.broadcasted_iota(jnp.int32, shape, 2).reshape(g * tb, keys)
        softmax_step(q, k_ref[r, 0, 0, :keys], v_ref[r, 0, 0, :keys], m_ref, l_ref, acc_ref, c, mask=ki <= ti)

    @pl.when(half == 0)
    def _():
        diagonal(n // 2)

    @pl.when(half == 1)
    def _():
        diagonal(n)

    den = jnp.sum(l_ref[...], axis=2, keepdims=True)
    o = (acc_ref[...] / den).astype(BF16)
    for j in range(g):
        o_ref[:, j * dh:(j + 1) * dh] = o[j]


def new_attn(idx, q, kv, m, l, acc, c):
    hq, n, dh = q.shape
    sp, _, nk, t, _ = kv.shape
    g = hq // nk
    st = pl.BlockSpec((g, TB, dh), lambda h, i, s: (h, i, 0))
    return pl.pallas_call(
        functools.partial(new_kernel, c=c),
        grid_spec=pltpu.PrefetchScalarGridSpec(
            num_scalar_prefetch=1,
            grid=(nk, n // TB),
            in_specs=[
                st,
                pl.BlockSpec((sp, 1, 1, t, dh), lambda h, i, s: (0, 0, h, 0, 0)),
                pl.BlockSpec((sp, 1, 1, t, dh), lambda h, i, s: (0, 1, h, 0, 0)),
                st, st, st,
            ],
            out_specs=pl.BlockSpec((TB, g * dh), lambda h, i, s: (i, h)),
            scratch_shapes=[pltpu.VMEM((g, TB, dh), F32)] * 3,
        ),
        out_shape=jax.ShapeDtypeStruct((n, hq * dh), BF16),
        compiler_params=params(2),
        cost_estimate=cost(8 * hq * n * sp * t * dh // 2, 3 * hq * n * dh * 4),
        name='new_attn',
    )(idx, q, kv, kv, m, l, acc)


def out_kernel(x_ref, a_ref, b_ref, wa_ref, wb_ref, o_ref):
    y = jnp.dot(a_ref[...], wa_ref[0], preferred_element_type=F32)
    y = y + jnp.dot(b_ref[...], wb_ref[...], preferred_element_type=F32)
    o_ref[...] = x_ref[...] + y.astype(BF16)


def out_proj(l, x, a, b, wa, wb):
    n, d = x.shape
    k = a.shape[1]
    return pl.pallas_call(
        out_kernel,
        grid=(d // OB,),
        in_specs=[
            pl.BlockSpec((n, OB), lambda i: (0, i)),
            pl.BlockSpec((n, k), lambda i: (0, 0)),
            pl.BlockSpec((n, k), lambda i: (0, 0)),
            pl.BlockSpec((1, k, OB), lambda i: (l, 0, i)),
            pl.BlockSpec((k, OB), lambda i: (0, i)),
        ],
        out_specs=pl.BlockSpec((n, OB), lambda i: (0, i)),
        out_shape=jax.ShapeDtypeStruct((n, d), BF16),
        compiler_params=params(),
        cost_estimate=cost(4 * n * k * d, 4 * k * d),
        name='out_proj',
    )(x, a, b, wa, wb)


def mlp_kernel(x_ref, g_ref, wg_ref, wu_ref, wd_ref, o_ref, h_ref, u_ref, a_ref, b_ref, *, nf):
    i = pl.program_id(0)

    def activate():
        a = a_ref[...].astype(F32)
        b = b_ref[...].astype(F32)
        j = jnp.maximum(i - 1, 0)
        u = a * (1.0 / (1.0 + jnp.exp(-a))) * b
        u_ref[:, pl.ds(pl.multiple_of(j * CB, CB), CB)] = u.astype(BF16)

    @pl.when(i == 0)
    def _():
        norm_into(h_ref, x_ref, g_ref)
        a_ref[...] = jnp.zeros_like(a_ref)
        b_ref[...] = jnp.zeros_like(b_ref)

    @pl.when(i < nf)
    def _():
        activate()
        a_ref[...] = jnp.dot(h_ref[...], wg_ref[0], preferred_element_type=F32).astype(BF16)
        b_ref[...] = jnp.dot(h_ref[...], wu_ref[0], preferred_element_type=F32).astype(BF16)

    @pl.when(i == nf)
    def _():
        activate()

    @pl.when(i >= nf)
    def _():
        o_ref[...] = jnp.dot(u_ref[...], wd_ref[0], preferred_element_type=F32)


def mlp(l, x, g, wg, wu, wd):
    n, d = x.shape
    f = wg.shape[-1]
    nf = f // CB
    fi = lambda i: jnp.minimum(i, nf - 1)
    di = lambda i: jnp.maximum(i - nf, 0)
    return pl.pallas_call(
        functools.partial(mlp_kernel, nf=nf),
        grid=(nf + d // DB,),
        in_specs=[
            pl.BlockSpec((n, d), lambda i: (0, 0)),
            pl.BlockSpec((1, 1, d), lambda i: (l, 0, 0)),
            pl.BlockSpec((1, d, CB), lambda i: (l, 0, fi(i))),
            pl.BlockSpec((1, d, CB), lambda i: (l, 0, fi(i))),
            pl.BlockSpec((1, f, DB), lambda i: (l, 0, di(i))),
        ],
        out_specs=pl.BlockSpec((n, DB), lambda i: (0, di(i))),
        out_shape=jax.ShapeDtypeStruct((n, d), F32),
        scratch_shapes=[
            pltpu.VMEM((n, d), BF16), pltpu.VMEM((n, f), BF16),
            pltpu.VMEM((n, CB), BF16), pltpu.VMEM((n, CB), BF16),
        ],
        compiler_params=params(),
        cost_estimate=cost(6 * n * d * f, 6 * d * f),
        name='mlp',
    )(x, g, wg, wu, wd)


def solution(mesh):
    sp = mesh.shape['sp']
    tp = mesh.shape['tp']
    row = ('dp', 'sp')
    kv_spec = P(None, row, 'tp', None)
    col = P(None, None, 'tp')
    rowsplit = P(None, 'tp', None)
    swap_perm = [(0, 1), (1, 0)]

    def swap(t):
        return lax.ppermute(t, 'tp', swap_perm)

    def after(t, *deps):
        return lax.optimization_barrier((t,) + deps)[0]

    def body(x, pos, k_hist, v_hist, wq, wk, wv, wo, wg, wu, wd, g1, g2):
        n, d = x.shape
        layers, _, nk, dh = k_hist.shape
        n2 = n // 2
        c = dh ** -0.5 * LOG2E
        r = lax.axis_index('sp')
        t = lax.axis_index('tp')
        g1 = g1[:, None, :]
        g2 = g2[:, None, :]

        half = dh // 2
        inv = ROPE_THETA ** (-(jnp.arange(half, dtype=F32) * (2.0 / dh)))
        ang = pos.astype(F32)[:, None] * inv
        cs, sn = jnp.cos(ang), jnp.sin(ang)
        cos = jnp.concatenate([cs, cs], axis=-1)
        sin = jnp.concatenate([-sn, sn], axis=-1)

        def own_other(a):
            return (lax.dynamic_slice_in_dim(a, t * n2, n2, axis=0),
                    lax.dynamic_slice_in_dim(a, (1 - t) * n2, n2, axis=0))

        def in_order(own, other, axis):
            both = jnp.concatenate([own, other], axis=axis)
            flip = jnp.concatenate([other, own], axis=axis)
            return jnp.where(t == 0, both, flip)

        cos_s, cos_p = own_other(cos)
        sin_s, sin_p = own_other(sin)
        x_s, x_p = own_other(x)
        idx_s = jnp.stack([r, t]).astype(jnp.int32)
        idx_p = jnp.stack([r, 1 - t]).astype(jnp.int32)

        hist = jnp.stack([k_hist, v_hist], axis=1).transpose(0, 1, 3, 2, 4)
        kq = wo.shape[1] // sp
        ks, vs = [], []
        hist_all = [lax.all_gather(hist[l], 'sp', axis=0) for l in range(layers)]

        def fetch_out(l, start, end):
            piece = lax.dynamic_slice_in_dim(after(wo, start)[l], r * kq, kq, axis=0)
            return after(swap(piece), end)

        def gather_out(piece):
            return lax.all_gather(piece, 'sp', axis=0, tiled=True)

        wo_next = None
        for l in range(layers):
            q_s, kv_s = qkv(l, x_s, g1, cos_s, sin_s, wq, wk, wv, dh)
            if l == 0:
                q_p, kv_p = qkv(l, x_p, g1, cos_p, sin_p, wq, wk, wv, dh)
                st_s = hist_attn(after(q_s, q_p), hist_all[l], c)
                wo_rem = gather_out(fetch_out(l, pos, st_s[0]))
            else:
                st_s = hist_attn(q_s, hist_all[l], c)
                x_p = after(x_p, st_s[0])
                q_p, kv_p = qkv(l, x_p, g1, cos_p, sin_p, wq, wk, wv, dh)
                wo_rem = wo_next
            kv = in_order(kv_s, kv_p, 2)
            ks.append(kv[0])
            vs.append(kv[1])
            kv_all = lax.all_gather(kv, 'sp', axis=0)
            st_p = hist_attn(after(q_p, st_s[0]), hist_all[l], c)
            q_s = after(q_s, st_p[0])
            o_s = new_attn(idx_s, q_s, kv_all, *st_s, c)
            q_p = after(q_p, o_s)
            if l + 1 < layers:
                piece = fetch_out(l + 1, st_s[0], o_s)
                q_p = after(q_p, piece)
                wo_next = gather_out(piece)
            o_p = new_attn(idx_p, q_p, kv_all, *st_p, c)
            r_p = swap(o_s)
            r_s = swap(o_p)
            x_p = out_proj(l, x_p, o_p, r_p, wo, wo_rem)
            part_p = mlp(l, x_p, g2, wg, wu, wd)
            x_s = after(x_s, part_p)
            x_s = out_proj(l, x_s, o_s, r_s, wo, wo_rem)
            part_s = mlp(l, x_s, g2, wg, wu, wd)
            recv = swap(part_p)
            x_s = x_s + (part_s + recv).astype(BF16)
            x_p = swap(x_s)
        x = in_order(x_s, x_p, 0)
        k = jnp.stack(ks).transpose(0, 2, 1, 3)
        v = jnp.stack(vs).transpose(0, 2, 1, 3)
        return x, k, v

    in_specs = (P(row, None), P(row), kv_spec, kv_spec, col, col, col, rowsplit, col, col, rowsplit, P(), P())
    out_specs = (P(row, None), kv_spec, kv_spec)
    return jax.shard_map(body, mesh=mesh, in_specs=in_specs, out_specs=out_specs, check_vma=False)
```
